32 devices in a mesh: grp: 2 (over x), row: 16 (over z, y, core).
Axes of the slice: x: 2, y: 2, z: 4, core: 2. Of those that a mesh axis runs over, the one named last changes fastest.
Arguments:
- tiles: bfloat16 [192, 512, 512], P(('grp', 'row')), may hold values from -0.15625 to 0.15625
- tile_row: int32 [192], P(('grp', 'row')), may hold values from 0 to 63, as said below
- tile_col: int32 [192], P(('grp', 'row')), may hold values from 0 to 63, as said below
- tile_count: int32 [32], P(('grp', 'row')), may hold values from 3 to 6, as said below
- q_block: bfloat16 [32768, 256], P(('grp', 'row')), may hold values from -80 to 80
Outputs:
- q_next: float32 [32768, 256], P(('grp', 'row'))
The draws below stay inside these ranges and needn't reach their ends.
Inputs may be any that keep to these rules, and one draw needn't show every extreme that they name: `tile_row`: each slot names one of its device's tile rows: d * 2 to d * 2 + 1 for device d. `tile_col`: each slot's tile column is (tile_row + o) mod 64 with o from minus 2 to 2; no two slots of one device name the same pair of tile row and tile column. `tile_count`: some device has all 6 slots live.
All inputs are finite; a program needn't handle non-finite values.
Results may differ from the reference program's by a relative error of at most 0.0029.
Values may be sent and summed in bfloat16 or wider, within the bound.
A program may use at most 64 MiB of HBM per device.

```python
import jax
import jax.numpy as jnp
from jax import lax

BS = 512
K = 256
TR = 2
H = 2
TILES_DEV = 6
NT = 64
N = 32768
N_GRP = 2
N_ROW = 16


def slot_pairs(key):
    device_total = N_GRP * N_ROW
    span = 2 * H + 1
    pair_total = TR * span
    keys = jax.random.split(jax.random.fold_in(key, 31), device_total)
    scores = jax.vmap(lambda single: jax.random.permutation(single, pair_total))(keys).astype(jnp.int32)
    pair_ids = jnp.arange(pair_total, dtype=jnp.int32)[None, :]
    first_pair = H - 1
    second_pair = (TR - 1) * span + H + 1
    third_pair = H
    scores = jnp.where(pair_ids == first_pair, -3, jnp.where(pair_ids == second_pair, -2, jnp.where(pair_ids == third_pair, -1, scores)))
    order = jnp.argsort(scores, axis=1, stable=True)[:, :TILES_DEV].astype(jnp.int32)
    local_row = order // span
    offset = order % span - H
    device = jnp.arange(device_total, dtype=jnp.int32)[:, None]
    rows = device * TR + local_row
    cols = (rows + offset) % (TR * device_total)
    return (rows.reshape(-1).astype(jnp.int32), cols.reshape(-1).astype(jnp.int32))


def draw_tile_row(key, part):
    rows, cols = slot_pairs(key)
    return rows


def draw_tile_col(key, part):
    rows, cols = slot_pairs(key)
    return cols


def draw_tile_count(key, part):
    device_total = N_GRP * N_ROW
    counts = jax.random.randint(jax.random.fold_in(key, 21), (device_total,), 3, TILES_DEV + 1, dtype=jnp.int32)
    busiest = jax.random.randint(jax.random.fold_in(key, 22), (), 0, device_total, dtype=jnp.int32)
    device_ids = jnp.arange(device_total, dtype=jnp.int32)
    return jnp.where(device_ids == busiest, TILES_DEV, counts).astype(jnp.int32)


def draw_q_block(key, part):
    row_tile = jnp.arange(N, dtype=jnp.int32) // BS
    row_scale = 10.0 ** (row_tile.astype(jnp.float32) / (NT - 1))
    base = jnp.clip(jax.random.normal(jax.random.fold_in(key, 43), (N, K), jnp.float32), -6.0, 6.0)
    return (base * row_scale[:, None]).astype(jnp.bfloat16)


def steps_of(stream_key, dims, cuts, low, high):
    level = 1.0
    for position, shards_of in cuts:
        draws = jax.random.uniform(jax.random.fold_in(jax.random.fold_in(stream_key, 6), position), (shards_of,), jnp.float32, low / len(cuts), high / len(cuts))
        level = level * jnp.repeat(jnp.exp(draws), dims[position] // shards_of).reshape((-1,) + (1,) * (len(dims) - 1 - position))
    return level


def centred(rng, shape, deviation, reach, cuts=(), held_as=jnp.bfloat16):
    gain = steps_of(rng, shape, cuts, -0.22, 0.18) if cuts else 1.0
    array = jax.random.normal(rng, shape, jnp.float32) * deviation * gain
    return jnp.minimum(jnp.maximum(array, -reach), reach).astype(held_as)


def setup_inputs(seed: int = 0) -> dict:
    key_of = jax.random.split(jax.random.key(seed), 6)
    tiles = centred(key_of[0], (N_GRP * N_ROW * TILES_DEV, BS, BS), (BS * TILES_DEV // TR) ** -0.5, 0.15625, ((0, 32),))
    tile_row = draw_tile_row(jax.random.fold_in(key_of[5], 71), 0)
    tile_col = draw_tile_col(jax.random.fold_in(key_of[5], 71), 0)
    tile_count = draw_tile_count(jax.random.fold_in(key_of[5], 71), 0)
    q_block = draw_q_block(jax.random.fold_in(key_of[5], 71), 0)
    return dict(tiles=tiles, tile_row=tile_row, tile_col=tile_col, tile_count=tile_count, q_block=q_block)


def reference(tiles, tile_row, tile_col, tile_count, q_block):
    device_total = N_GRP * N_ROW
    tile_sets = tiles.reshape(device_total, TILES_DEV, BS, BS)
    slot_rows = tile_row.reshape(device_total, TILES_DEV)
    slot_cols = tile_col.reshape(device_total, TILES_DEV)
    q_tiles = q_block.astype(jnp.float32).reshape(NT, BS, K)
    slot_ids = jnp.arange(TILES_DEV, dtype=jnp.int32)
    row_ids = jnp.arange(TR, dtype=jnp.int32)
    column_ids = jnp.arange(TR + 2 * H, dtype=jnp.int32)

    def forward(device):
        live_slot = slot_ids < tile_count[device]
        local_row = (slot_rows[device] - device * TR).astype(jnp.int32)
        blocks = q_tiles[slot_cols[device]]
        products = jnp.einsum('sab,sbk->sak', tile_sets[device].astype(jnp.float32), blocks, precision=lax.Precision.HIGHEST)
        placing = ((local_row[None, :] == row_ids[:, None]) & live_slot[None, :]).astype(jnp.float32)
        return jnp.einsum('rs,sak->rak', placing, products, precision=lax.Precision.HIGHEST)
    aq_tiles = lax.map(forward, jnp.arange(device_total, dtype=jnp.int32)).reshape(NT, BS, K).astype(jnp.bfloat16)

    def backward(device):
        live_slot = slot_ids < tile_count[device]
        local_col = ((slot_cols[device] - device * TR + H) % NT).astype(jnp.int32)
        row_part = aq_tiles[slot_rows[device]].astype(jnp.float32)
        images = jnp.einsum('sab,sak->sbk', tile_sets[device].astype(jnp.float32), row_part, precision=lax.Precision.HIGHEST)
        placing = ((local_col[None, :] == column_ids[:, None]) & live_slot[None, :]).astype(jnp.float32)
        sums = jnp.einsum('cs,sbk->cbk', placing, images, precision=lax.Precision.HIGHEST)
        return (sums[H:H + TR], sums[:H].astype(jnp.bfloat16), sums[H + TR:].astype(jnp.bfloat16))
    own_part, lower, upper = lax.map(backward, jnp.arange(device_total, dtype=jnp.int32))
    lower, upper = lax.optimization_barrier((lower, upper))
    from_above = jnp.roll(lower, -1, axis=0).astype(jnp.float32)
    from_below = jnp.roll(upper, 1, axis=0).astype(jnp.float32)
    own_part = own_part.at[:, TR - H:].add(from_above)
    own_part = own_part.at[:, :H].add(from_below)
    y_full = own_part.reshape(N, K)
    gram_matrix = jnp.dot(y_full.T.astype(jnp.float32), y_full.astype(jnp.float32), precision=lax.Precision.HIGHEST, preferred_element_type=jnp.float32) / N
    factor_low = jnp.linalg.cholesky(gram_matrix)
    return lax.linalg.triangular_solve(factor_low, y_full, left_side=False, lower=True, transpose_a=True)
```

```python
import functools

import jax
import jax.numpy as jnp
from jax import lax
from jax.experimental import pallas as pl
from jax.experimental.pallas import tpu as pltpu
from jax.sharding import PartitionSpec as P

H = 2
BLOCK = 128
CHUNKS = 2
DIRECT_LIMIT = 32
MESH = pl.DeviceIdType.MESH
F32 = jnp.float32
BF16 = jnp.bfloat16
EXACT = lax.Precision.HIGHEST


def split_high_low(x):
    high = x.astype(BF16)
    return high, (x - high.astype(F32)).astype(BF16)


def dot(a, b, dims, precision=None):
    return lax.dot_general(
        a, b, (dims, ((), ())), precision=precision, preferred_element_type=F32
    )


NN = ((1,), (0,))
NT = ((1,), (1,))
TN = ((0,), (0,))


def dot_split(x, m, dims):
    xh, xl = split_high_low(x)
    mh, ml = split_high_low(m)
    return dot(xh, mh, dims) + (dot(xl, mh, dims) + dot(xh, ml, dims))


def on_ring(device, rows):
    return (device // rows, device % rows)


def step_kernel(
    direct, groups, rows, tile_total,
    row_ref, col_ref, count_ref, tiles_hbm, q_hbm,
    y_hbm, gram_ref,
    window, tiles, tiles_t, aq, send_lo, send_hi, recv_lo, recv_hi, y, acc, pair, shards,
    load_sems, q_sems, y_sems, pair_sems, rs_sems, ag_sems, out_sem,
):
    slots = tiles_hbm.shape[0]
    size = tiles_hbm.shape[1]
    own = q_hbm.shape[0] // size
    chunks = window.shape[0]
    width = window.shape[2]
    span = 2 * H + 1
    edge = H * size
    inner = own * size
    total = groups * rows
    g, r = lax.axis_index("grp"), lax.axis_index("row")
    me = g * rows + r
    nxt = on_ring((me + 1) % total, rows)
    prv = on_ring((me + total - 1) % total, rows)
    chips = total // 2
    parity = r % 2
    chip = me // 2
    mate = on_ring(chip * 2 + (1 - parity), rows)

    def peer(offset):
        return on_ring(((chip + offset) % chips) * 2 + parity, rows)

    loads = []
    for k in range(chunks):
        loads.append(pltpu.make_async_copy(
            q_hbm.at[:, pl.ds(k * width, width)],
            window.at[k, pl.ds(edge, inner)], load_sems.at[slots + k]))
        loads[-1].start()
    tile_loads = []
    for s in range(slots):
        tile_loads.append(pltpu.make_async_copy(tiles_hbm.at[s], tiles.at[s], load_sems.at[s]))
        tile_loads[-1].start()

    barrier = pltpu.get_barrier_semaphore()
    if direct:
        for other in range(1, total):
            pl.semaphore_signal(
                barrier, inc=1, device_id=on_ring((me + other) % total, rows),
                device_id_type=MESH)
        pl.semaphore_wait(barrier, total - 1)
    else:
        for other in (nxt, prv):
            pl.semaphore_signal(barrier, inc=1, device_id=other, device_id_type=MESH)
        pl.semaphore_wait(barrier, 2)

    def remote(src, dst, sems, index, device):
        return pltpu.make_async_remote_copy(
            src_ref=src, dst_ref=dst, send_sem=sems.at[0, index], recv_sem=sems.at[1, index],
            device_id=device, device_id_type=MESH)

    halo = []
    for k in range(chunks):
        loads[k].wait()
        up = remote(window.at[k, pl.ds(edge + inner - edge, edge)],
                    window.at[k, pl.ds(0, edge)], q_sems, 2 * k, nxt)
        down = remote(window.at[k, pl.ds(edge, edge)],
                      window.at[k, pl.ds(edge + inner, edge)], q_sems, 2 * k + 1, prv)
        up.start()
        down.start()
        halo.append((up, down))

    tiles[slots] = jnp.zeros((size, size), BF16)
    tiles_t[slots] = jnp.zeros((size, size), BF16)
    for s in range(slots):
        tile_loads[s].wait()
        tiles_t[s] = tiles[s].T

    slot_of = {}
    for row in range(own):
        for off in range(span):
            slot_of[row, off] = jnp.int32(slots)
    for s in range(slots):
        live = s < count_ref[0]
        at_row = row_ref[s] % own
        offset = (col_ref[s] - row_ref[s] + H + tile_total) % tile_total
        for row in range(own):
            for off in range(span):
                hit = live & (at_row == row) & (offset == off)
                slot_of[row, off] = jnp.where(hit, jnp.int32(s), slot_of[row, off])

    def terms(column):
        value = None
        for row in range(own):
            off = column - row
            if 0 <= off < span:
                part = dot(tiles_t[slot_of[row, off]], aq[row], NN)
                value = part if value is None else value + part
        return value

    rim = []
    for k in range(chunks):
        for copy in halo[k]:
            copy.wait_recv()
        for row in range(own):
            value = None
            for off in range(span):
                part = dot(tiles[slot_of[row, off]],
                           window[k, pl.ds((row + off) * size, size)], NN)
                value = part if value is None else value + part
            aq[row] = value.astype(BF16)
        for column in range(H):
            send_lo[k, pl.ds(column * size, size)] = terms(column).astype(BF16)
        down = remote(send_lo.at[k], recv_lo.at[k], y_sems, 2 * k, prv)
        down.start()
        for column in range(H):
            send_hi[k, pl.ds(column * size, size)] = terms(H + own + column).astype(BF16)
        up = remote(send_hi.at[k], recv_hi.at[k], y_sems, 2 * k + 1, nxt)
        up.start()
        rim.append((down, up))
        for column in range(own):
            y[k, pl.ds(column * size, size)] = terms(H + column)

    writes = []
    halves = []
    for k in range(chunks):
        rim[k][1].wait_recv()
        y[k, pl.ds(0, edge)] = y[k, pl.ds(0, edge)] + recv_hi[k].astype(F32)
        rim[k][0].wait_recv()
        y[k, pl.ds(inner - edge, edge)] = (
            y[k, pl.ds(inner - edge, edge)] + recv_lo[k].astype(F32))
        write = pltpu.make_async_copy(y.at[k], y_hbm.at[k], out_sem.at[k])
        write.start()
        writes.append(write)
        high, low = split_high_low(y[k])
        halves.append((high, low))
        for j in range(k + 1):
            jh, jl = halves[j]
            block = dot(jh, high, TN) + (dot(jh, low, TN) + dot(jl, high, TN))
            acc[k, pl.ds(j * width, width)] = block
            if j != k:
                acc[j, pl.ds(k * width, width)] = block.T

    if direct:
        rows_of = acc.shape[1] // chips
        trade = remote(acc.at[1 - parity], pair, pair_sems, 0, mate)
        trade.start()
        trade.wait()
        acc[parity] = acc[parity] + pair[...]
        scatter = []
        for o in range(1, chips):
            at = pl.multiple_of(((chip + o) % chips) * rows_of, rows_of)
            copy = remote(acc.at[parity, pl.ds(at, rows_of)], shards.at[o], rs_sems, o, peer(o))
            copy.start()
            scatter.append(copy)
        here = pl.multiple_of(chip * rows_of, rows_of)
        value = acc[parity, pl.ds(here, rows_of)]
        for o in range(1, chips):
            scatter[o - 1].wait_recv()
            value = value + shards[o]
        gram_ref[parity, pl.ds(here, rows_of)] = value
        gather = []
        for o in range(1, chips):
            copy = remote(gram_ref.at[parity, pl.ds(here, rows_of)],
                          gram_ref.at[parity, pl.ds(here, rows_of)], ag_sems, o, peer(o))
            copy.start()
            gather.append(copy)
        for o in range(1, chips):
            at = pl.multiple_of(((chip + chips - o) % chips) * rows_of, rows_of)
            remote(gram_ref.at[parity, pl.ds(here, rows_of)],
                   gram_ref.at[parity, pl.ds(at, rows_of)], ag_sems, o, peer(o)).wait_recv()
        back = remote(gram_ref.at[parity], gram_ref.at[parity], pair_sems, 1, mate)
        back.start()
        remote(gram_ref.at[parity], gram_ref.at[1 - parity], pair_sems, 1, mate).wait_recv()
        back.wait_send()
        for copy in scatter + gather:
            copy.wait_send()
    else:
        gram_ref[...] = acc[...]
    for k in range(chunks):
        for copy in halo[k] + rim[k]:
            copy.wait_send()
        writes[k].wait()


def inverse_factor(a):
    size = a.shape[0]
    groups = size // 8
    parts = [a[8 * i : 8 * i + 8] for i in range(groups)]
    lane = lax.broadcasted_iota(jnp.int32, (8, size), 1)
    sub = lax.broadcasted_iota(jnp.int32, (8, size), 0)
    pivots = [None] * groups
    for j in range(size):
        home, at = divmod(j, 8)
        columns = [
            jnp.broadcast_to(parts[i][:, j : j + 1], (8, size)) for i in range(home, groups)
        ]
        pivot = jnp.broadcast_to(columns[0][at : at + 1], (8, size))
        row = jnp.broadcast_to(parts[home][at : at + 1], (8, size))
        row = jnp.where(lane == j, 1.0, row) * (1.0 / pivot)
        prior = pivots[home]
        pivots[home] = pivot if prior is None else jnp.where(sub == at, pivot, prior)
        for i in range(home, groups):
            if i == home and at == 7:
                continue
            kept = jnp.where(lane == j, 0.0, parts[i])
            new = kept - columns[i - home] * row
            if i == home:
                new = jnp.where(sub > at, new, parts[i])
            parts[i] = new
    whole = []
    for i in range(groups):
        rows = sub + 8 * i
        unit = jnp.where(lane < rows, parts[i], jnp.where(lane == rows, 1.0, 0.0))
        whole.append(unit * lax.rsqrt(pivots[i]))
    return jnp.concatenate(whole, axis=0)


def solve_kernel(scale, y_hbm, gram_ref, out_hbm, y, out, in_sems, out_sems):
    blocks = y_hbm.shape[0]
    width = y_hbm.shape[2]
    reads = []
    for k in range(blocks):
        reads.append(pltpu.make_async_copy(y_hbm.at[k], y.at[k], in_sems.at[k]))
        reads[-1].start()
    gram = [
        [gram_ref[j, i * width : (i + 1) * width] * scale for j in range(blocks)]
        for i in range(blocks)
    ]
    for read in reads:
        read.wait()
    writes = []
    for k in range(blocks):
        inverse = inverse_factor(gram[k][k])
        basis = dot_split(y[k], inverse, NT)
        out[k] = basis
        write = pltpu.make_async_copy(
            out.at[k], out_hbm.at[:, pl.ds(k * width, width)], out_sems.at[k])
        write.start()
        writes.append(write)
        over = {j: dot(inverse, gram[k][j], NN, EXACT) for j in range(k + 1, blocks)}
        for i in range(k + 1, blocks):
            for j in range(i, blocks):
                gram[i][j] = gram[i][j] - dot(over[i], over[j], TN, EXACT)
            y[i] = y[i] - dot_split(basis, over[i], NN)
    for write in writes:
        write.wait()


def on_device(tiles, tile_row, tile_col, tile_count, q_block):
    slots, size, unused_size = tiles.shape
    height, basis = q_block.shape
    groups, rows = lax.axis_size("grp"), lax.axis_size("row")
    total = groups * rows
    own = height // size
    tile_total = own * total
    width = BLOCK
    chunks = basis // width
    edge = H * size
    direct = total <= DIRECT_LIMIT and (basis // (total // 2)) % 8 == 0
    chips = max(total // 2, 1)
    shard = basis // chips if direct else 8
    any_spec = pl.BlockSpec(memory_space=pl.ANY)
    vmem_spec = pl.BlockSpec(memory_space=pltpu.VMEM)
    smem_spec = pl.BlockSpec(memory_space=pltpu.SMEM)
    dma = pltpu.SemaphoreType.DMA
    y, gram = pl.pallas_call(
        functools.partial(step_kernel, direct, groups, rows, tile_total),
        out_shape=(
            jax.ShapeDtypeStruct((chunks, height, width), F32),
            jax.ShapeDtypeStruct((chunks, basis, width), F32),
        ),
        in_specs=[smem_spec, smem_spec, smem_spec, any_spec, any_spec],
        out_specs=(any_spec, vmem_spec),
        scratch_shapes=[
            pltpu.VMEM((chunks, height + 2 * edge, width), BF16),
            pltpu.VMEM((slots + 1, size, size), BF16),
            pltpu.VMEM((slots + 1, size, size), BF16),
            pltpu.VMEM((own, size, width), BF16),
            pltpu.VMEM((chunks, edge, width), BF16),
            pltpu.VMEM((chunks, edge, width), BF16),
            pltpu.VMEM((chunks, edge, width), BF16),
            pltpu.VMEM((chunks, edge, width), BF16),
            pltpu.VMEM((chunks, height, width), F32),
            pltpu.VMEM((chunks, basis, width), F32),
            pltpu.VMEM((basis, width), F32),
            pltpu.VMEM((chips if direct else 1, shard, width), F32),
            dma((slots + chunks,)),
            dma((2, 2 * chunks)),
            dma((2, 2 * chunks)),
            dma((2, 2)),
            dma((2, chips if direct else 1)),
            dma((2, chips if direct else 1)),
            dma((chunks,)),
        ],
        compiler_params=pltpu.CompilerParams(
            collective_id=0, has_side_effects=True, vmem_limit_bytes=40 * 2**20
        ),
    )(tile_row, tile_col, tile_count, tiles, q_block)
    if not direct:
        gram = lax.psum(gram, ("grp", "row"))
    return pl.pallas_call(
        functools.partial(solve_kernel, 1.0 / (height * total)),
        out_shape=jax.ShapeDtypeStruct((height, basis), F32),
        in_specs=[any_spec, vmem_spec],
        out_specs=any_spec,
        scratch_shapes=[
            pltpu.VMEM((chunks, height, width), F32),
            pltpu.VMEM((chunks, height, width), F32),
            dma((chunks,)),
            dma((chunks,)),
        ],
        compiler_params=pltpu.CompilerParams(vmem_limit_bytes=40 * 2**20),
    )(y, gram)


def solution(mesh):
    placed = (
        P(("grp", "row"), None, None),
        P(("grp", "row")),
        P(("grp", "row")),
        P(("grp", "row")),
        P(("grp", "row"), None),
    )
    return jax.shard_map(
        on_device, mesh=mesh, in_specs=placed, out_specs=P(("grp", "row"), None), check_vma=False
    )
```

```python
import functools

import jax
import jax.numpy as jnp
from jax import lax
from jax.experimental import pallas as pl
from jax.experimental.pallas import tpu as pltpu
from jax.sharding import PartitionSpec as P

H = 2
BLOCK = 128
CHUNKS = 2
DIRECT_LIMIT = 32
VMEM_LIMIT = 67_043_328
MESH = pl.DeviceIdType.MESH
F32 = jnp.float32
BF16 = jnp.bfloat16
EXACT = lax.Precision.HIGHEST


def split_high_low(x):
    high = x.astype(BF16)
    return high, (x - high.astype(F32)).astype(BF16)


def dot(a, b, dims, precision=None):
    return lax.dot_general(
        a, b, (dims, ((), ())), precision=precision, preferred_element_type=F32
    )


NN = ((1,), (0,))
NT = ((1,), (1,))
TN = ((0,), (0,))


def dot_split(x, m, dims):
    xh, xl = split_high_low(x)
    mh, ml = split_high_low(m)
    return dot(xh, mh, dims) + (dot(xl, mh, dims) + dot(xh, ml, dims))


def on_ring(device, rows):
    return (device // rows, device % rows)


def step_kernel(
    direct, groups, rows, tile_total,
    row_hbm, col_hbm, count_hbm, tiles_hbm, q_hbm,
    y_hbm, gram_ref,
    row_ref, col_ref, count_ref, window, tiles, tiles_t, aq, send_lo, send_hi, recv_lo, recv_hi, y, acc, pair, shards,
    load_sems, q_sems, y_sems, pair_sems, rs_sems, ag_sems, out_sem, index_sems,
):
    slots = tiles_hbm.shape[0]
    size = tiles_hbm.shape[1]
    own = q_hbm.shape[0] // size
    chunks = window.shape[0]
    width = window.shape[2]
    span = 2 * H + 1
    edge = H * size
    inner = own * size
    total = groups * rows
    g, r = lax.axis_index("grp"), lax.axis_index("row")
    me = g * rows + r
    nxt = on_ring((me + 1) % total, rows)
    prv = on_ring((me + total - 1) % total, rows)
    chips = total // 2
    parity = r % 2
    chip = me // 2
    mate = on_ring(chip * 2 + (1 - parity), rows)

    def peer(offset):
        return on_ring(((chip + offset) % chips) * 2 + parity, rows)

    loads = []
    for k in range(chunks):
        loads.append(pltpu.make_async_copy(
            q_hbm.at[:, pl.ds(k * width, width)],
            window.at[k, pl.ds(edge, inner)], load_sems.at[slots + k]))
        loads[-1].start()
    tile_loads = []
    for s in range(slots):
        tile_loads.append(pltpu.make_async_copy(tiles_hbm.at[s], tiles.at[s], load_sems.at[s]))
        tile_loads[-1].start()

    index_loads = []
    for k, (src, dst) in enumerate(
        ((row_hbm, row_ref), (col_hbm, col_ref), (count_hbm, count_ref))
    ):
        index_loads.append(pltpu.make_async_copy(src, dst, index_sems.at[k]))
        index_loads[-1].start()

    barrier = pltpu.get_barrier_semaphore()
    if direct:
        for other in range(1, total):
            pl.semaphore_signal(
                barrier, inc=1, device_id=on_ring((me + other) % total, rows),
                device_id_type=MESH)
        pl.semaphore_wait(barrier, total - 1)
    else:
        for other in (nxt, prv):
            pl.semaphore_signal(barrier, inc=1, device_id=other, device_id_type=MESH)
        pl.semaphore_wait(barrier, 2)

    def remote(src, dst, sems, index, device):
        return pltpu.make_async_remote_copy(
            src_ref=src, dst_ref=dst, send_sem=sems.at[0, index], recv_sem=sems.at[1, index],
            device_id=device, device_id_type=MESH)

    halo = []
    for k in range(chunks):
        loads[k].wait()
        up = remote(window.at[k, pl.ds(edge + inner - edge, edge)],
                    window.at[k, pl.ds(0, edge)], q_sems, 2 * k, nxt)
        down = remote(window.at[k, pl.ds(edge, edge)],
                      window.at[k, pl.ds(edge + inner, edge)], q_sems, 2 * k + 1, prv)
        up.start()
        down.start()
        halo.append((up, down))

    tiles[slots] = jnp.zeros((size, size), BF16)
    tiles_t[slots] = jnp.zeros((size, size), BF16)
    for s in range(slots):
        tile_loads[s].wait()
        tiles_t[s] = tiles[s].T

    for load in index_loads:
        load.wait()
    slot_of = {}
    for row in range(own):
        for off in range(span):
            slot_of[row, off] = jnp.int32(slots)
    for s in range(slots):
        live = s < count_ref[0]
        at_row = row_ref[s] % own
        offset = (col_ref[s] - row_ref[s] + H + tile_total) % tile_total
        for row in range(own):
            for off in range(span):
                hit = live & (at_row == row) & (offset == off)
                slot_of[row, off] = jnp.where(hit, jnp.int32(s), slot_of[row, off])

    def terms(column):
        value = None
        for row in range(own):
            off = column - row
            if 0 <= off < span:
                part = dot(tiles_t[slot_of[row, off]], aq[row], NN)
                value = part if value is None else value + part
        return value

    rim = []
    for k in range(chunks):
        for copy in halo[k]:
            copy.wait_recv()
        for row in range(own):
            value = None
            for off in range(span):
                part = dot(tiles[slot_of[row, off]],
                           window[k, pl.ds((row + off) * size, size)], NN)
                value = part if value is None else value + part
            aq[row] = value.astype(BF16)
        for column in range(H):
            send_lo[k, pl.ds(column * size, size)] = terms(column).astype(BF16)
        down = remote(send_lo.at[k], recv_lo.at[k], y_sems, 2 * k, prv)
        down.start()
        for column in range(H):
            send_hi[k, pl.ds(column * size, size)] = terms(H + own + column).astype(BF16)
        up = remote(send_hi.at[k], recv_hi.at[k], y_sems, 2 * k + 1, nxt)
        up.start()
        rim.append((down, up))
        for column in range(own):
            y[k, pl.ds(column * size, size)] = terms(H + column)

    writes = []
    halves = []
    for k in range(chunks):
        rim[k][1].wait_recv()
        y[k, pl.ds(0, edge)] = y[k, pl.ds(0, edge)] + recv_hi[k].astype(F32)
        rim[k][0].wait_recv()
        y[k, pl.ds(inner - edge, edge)] = (
            y[k, pl.ds(inner - edge, edge)] + recv_lo[k].astype(F32))
        write = pltpu.make_async_copy(y.at[k], y_hbm.at[k], out_sem.at[k])
        write.start()
        writes.append(write)
        high, low = split_high_low(y[k])
        halves.append((high, low))
        for j in range(k + 1):
            jh, jl = halves[j]
            block = dot(jh, high, TN) + (dot(jh, low, TN) + dot(jl, high, TN))
            acc[k, pl.ds(j * width, width)] = block
            if j != k:
                acc[j, pl.ds(k * width, width)] = block.T

    if direct:
        rows_of = acc.shape[1] // chips
        trade = remote(acc.at[1 - parity], pair, pair_sems, 0, mate)
        trade.start()
        trade.wait()
        acc[parity] = acc[parity] + pair[...]
        scatter = []
        for o in range(1, chips):
            at = pl.multiple_of(((chip + o) % chips) * rows_of, rows_of)
            copy = remote(acc.at[parity, pl.ds(at, rows_of)], shards.at[o], rs_sems, o, peer(o))
            copy.start()
            scatter.append(copy)
        here = pl.multiple_of(chip * rows_of, rows_of)
        value = acc[parity, pl.ds(here, rows_of)]
        for o in range(1, chips):
            scatter[o - 1].wait_recv()
            value = value + shards[o]
        gram_ref[parity, pl.ds(here, rows_of)] = value
        gather = []
        for o in range(1, chips):
            copy = remote(gram_ref.at[parity, pl.ds(here, rows_of)],
                          gram_ref.at[parity, pl.ds(here, rows_of)], ag_sems, o, peer(o))
            copy.start()
            gather.append(copy)
        for o in range(1, chips):
            at = pl.multiple_of(((chip + chips - o) % chips) * rows_of, rows_of)
            remote(gram_ref.at[parity, pl.ds(here, rows_of)],
                   gram_ref.at[parity, pl.ds(at, rows_of)], ag_sems, o, peer(o)).wait_recv()
        back = remote(gram_ref.at[parity], gram_ref.at[parity], pair_sems, 1, mate)
        back.start()
        remote(gram_ref.at[parity], gram_ref.at[1 - parity], pair_sems, 1, mate).wait_recv()
        back.wait_send()
        for copy in scatter + gather:
            copy.wait_send()
    else:
        gram_ref[...] = acc[...]
    for k in range(chunks):
        for copy in halo[k] + rim[k]:
            copy.wait_send()
        writes[k].wait()


def inverse_factor(a):
    size = a.shape[0]
    groups = size // 8
    parts = [a[8 * i : 8 * i + 8] for i in range(groups)]
    lane = lax.broadcasted_iota(jnp.int32, (8, size), 1)
    sub = lax.broadcasted_iota(jnp.int32, (8, size), 0)

    def row_of(x, at):
        return jnp.broadcast_to(x[at : at + 1], (8, size))

    whole = []
    for home in range(groups):
        first = 8 * home
        later = range(home, groups)
        columns = [
            {i: jnp.broadcast_to(parts[i][:, first + l : first + l + 1], (8, size)) for i in later}
            for l in range(8)
        ]
        mine = parts[home]
        rows = []
        pivots = None
        for j in range(8):
            top = columns[j][home]
            pivot = row_of(top, j)
            inv = 1.0 / pivot
            pivots = pivot if pivots is None else jnp.where(sub == j, pivot, pivots)
            row = jnp.where(lane == first + j, 1.0, row_of(mine, j)) * inv
            rows.append(jnp.where((lane > first + j) & (lane < first + 8), 0.0, row))
            mine = jnp.where(
                sub > j, jnp.where(lane == first + j, 0.0, mine) - top * row, mine)
            for l in range(j + 1, 8):
                weight = row_of(top, l) * inv
                for i in later:
                    columns[l][i] = columns[l][i] - columns[j][i] * weight
        for i in later:
            if i > home:
                value = jnp.where((lane >= first) & (lane < first + 8), 0.0, parts[i])
                for j in range(8):
                    value = value - columns[j][i] * rows[j]
                parts[i] = value
        at = sub + first
        unit = jnp.where(lane < at, mine, jnp.where(lane == at, 1.0, 0.0))
        whole.append(unit * lax.rsqrt(pivots))
    return jnp.concatenate(whole, axis=0)


def solve_kernel(scale, y_hbm, gram_ref, out_hbm, y, out, in_sems, out_sems):
    blocks = y_hbm.shape[0]
    width = y_hbm.shape[2]
    reads = []
    for k in range(blocks):
        reads.append(pltpu.make_async_copy(y_hbm.at[k], y.at[k], in_sems.at[k]))
        reads[-1].start()
    gram = [
        [gram_ref[j, i * width : (i + 1) * width] * scale for j in range(blocks)]
        for i in range(blocks)
    ]
    for read in reads:
        read.wait()
    writes = []
    for k in range(blocks):
        inverse = inverse_factor(gram[k][k])
        basis = dot_split(y[k], inverse, NT)
        out[k] = basis
        write = pltpu.make_async_copy(
            out.at[k], out_hbm.at[:, pl.ds(k * width, width)], out_sems.at[k])
        write.start()
        writes.append(write)
        over = {j: dot(inverse, gram[k][j], NN, EXACT) for j in range(k + 1, blocks)}
        for i in range(k + 1, blocks):
            for j in range(i, blocks):
                gram[i][j] = gram[i][j] - dot(over[i], over[j], TN, EXACT)
            y[i] = y[i] - dot_split(basis, over[i], NN)
    for write in writes:
        write.wait()


def on_device(tiles, tile_row, tile_col, tile_count, q_block):
    slots, size, unused_size = tiles.shape
    height, basis = q_block.shape
    groups, rows = lax.axis_size("grp"), lax.axis_size("row")
    total = groups * rows
    own = height // size
    tile_total = own * total
    width = BLOCK
    chunks = basis // width
    edge = H * size
    direct = total <= DIRECT_LIMIT and (basis // (total // 2)) % 8 == 0
    chips = max(total // 2, 1)
    shard = basis // chips if direct else 8
    any_spec = pl.BlockSpec(memory_space=pl.ANY)
    vmem_spec = pl.BlockSpec(memory_space=pltpu.VMEM)
    hbm_spec = pl.BlockSpec(memory_space=pltpu.HBM)
    dma = pltpu.SemaphoreType.DMA
    y, gram = pl.pallas_call(
        functools.partial(step_kernel, direct, groups, rows, tile_total),
        out_shape=(
            jax.ShapeDtypeStruct((chunks, height, width), F32),
            jax.ShapeDtypeStruct((chunks, basis, width), F32),
        ),
        in_specs=[hbm_spec] * 5,
        out_specs=(any_spec, vmem_spec),
        scratch_shapes=[
            pltpu.SMEM(tile_row.shape, jnp.int32),
            pltpu.SMEM(tile_col.shape, jnp.int32),
            pltpu.SMEM(tile_count.shape, jnp.int32),
            pltpu.VMEM((chunks, height + 2 * edge, width), BF16),
            pltpu.VMEM((slots + 1, size, size), BF16),
            pltpu.VMEM((slots + 1, size, size), BF16),
            pltpu.VMEM((own, size, width), BF16),
            pltpu.VMEM((chunks, edge, width), BF16),
            pltpu.VMEM((chunks, edge, width), BF16),
            pltpu.VMEM((chunks, edge, width), BF16),
            pltpu.VMEM((chunks, edge, width), BF16),
            pltpu.VMEM((chunks, height, width), F32),
            pltpu.VMEM((chunks, basis, width), F32),
            pltpu.VMEM((basis, width), F32),
            pltpu.VMEM((chips if direct else 1, shard, width), F32),
            dma((slots + chunks,)),
            dma((2, 2 * chunks)),
            dma((2, 2 * chunks)),
            dma((2, 2)),
            dma((2, chips if direct else 1)),
            dma((2, chips if direct else 1)),
            dma((chunks,)),
            dma((3,)),
        ],
        compiler_params=pltpu.CompilerParams(
            collective_id=0, has_side_effects=True, vmem_limit_bytes=VMEM_LIMIT
        ),
    )(tile_row, tile_col, tile_count, tiles, q_block)
    if not direct:
        gram = lax.psum(gram, ("grp", "row"))
    return pl.pallas_call(
        functools.partial(solve_kernel, 1.0 / (height * total)),
        out_shape=jax.ShapeDtypeStruct((height, basis), F32),
        in_specs=[any_spec, vmem_spec],
        out_specs=any_spec,
        scratch_shapes=[
            pltpu.VMEM((chunks, height, width), F32),
            pltpu.VMEM((chunks, height, width), F32),
            dma((chunks,)),
            dma((chunks,)),
        ],
        compiler_params=pltpu.CompilerParams(vmem_limit_bytes=VMEM_LIMIT),
    )(y, gram)


def solution(mesh):
    placed = (
        P(("grp", "row"), None, None),
        P(("grp", "row")),
        P(("grp", "row")),
        P(("grp", "row")),
        P(("grp", "row"), None),
    )
    return jax.shard_map(
        on_device, mesh=mesh, in_specs=placed, out_specs=P(("grp", "row"), None), check_vma=False
    )
```

```python
import functools

import jax
import jax.numpy as jnp
from jax import lax
from jax.experimental import pallas as pl
from jax.experimental.pallas import tpu as pltpu
from jax.sharding import PartitionSpec as P

H = 2
BLOCK = 128
CHUNKS = 2
DIRECT_LIMIT = 32
VMEM_LIMIT = 67_043_328
MESH = pl.DeviceIdType.MESH
F32 = jnp.float32
BF16 = jnp.bfloat16
EXACT = lax.Precision.HIGHEST


def split_high_low(x):
    high = x.astype(BF16)
    return high, (x - high.astype(F32)).astype(BF16)


def dot(a, b, dims, precision=None):
    return lax.dot_general(
        a, b, (dims, ((), ())), precision=precision, preferred_element_type=F32
    )


NN = ((1,), (0,))
NT = ((1,), (1,))
TN = ((0,), (0,))


def dot_split(x, m, dims):
    xh, xl = split_high_low(x)
    mh, ml = split_high_low(m)
    return dot(xh, mh, dims) + (dot(xl, mh, dims) + dot(xh, ml, dims))


def on_ring(device, rows):
    return (device // rows, device % rows)


def step_kernel(
    direct, scale, groups, rows, tile_total,
    row_hbm, col_hbm, count_hbm, tiles_hbm, q_hbm,
    y_hbm, gram_ref, inverse_ref,
    row_ref, col_ref, count_ref, window, tiles, tiles_t, aq, send_lo, send_hi, recv_lo, recv_hi, y, acc, pair, shards,
    acc_first, gram_first, shards_first, swap, load_sems, q_sems, y_sems, pair_sems, rs_sems, ag_sems, rs_first, ag_first, out_sem, index_sems,
):
    slots = tiles_hbm.shape[0]
    size = tiles_hbm.shape[1]
    own = q_hbm.shape[0] // size
    chunks = window.shape[0]
    width = window.shape[2]
    span = 2 * H + 1
    edge = H * size
    inner = own * size
    total = groups * rows
    g, r = lax.axis_index("grp"), lax.axis_index("row")
    me = g * rows + r
    nxt = on_ring((me + 1) % total, rows)
    prv = on_ring((me + total - 1) % total, rows)
    chips = total // 2
    parity = r % 2
    chip = me // 2
    mate = on_ring(chip * 2 + (1 - parity), rows)

    def peer(offset):
        return on_ring(((chip + offset) % chips) * 2 + parity, rows)

    loads = []
    for k in range(chunks):
        loads.append(pltpu.make_async_copy(
            q_hbm.at[:, pl.ds(k * width, width)],
            window.at[k, pl.ds(edge, inner)], load_sems.at[slots + k]))
        loads[-1].start()
    tile_loads = []
    for s in range(slots):
        tile_loads.append(pltpu.make_async_copy(tiles_hbm.at[s], tiles.at[s], load_sems.at[s]))
        tile_loads[-1].start()

    index_loads = []
    for k, (src, dst) in enumerate(
        ((row_hbm, row_ref), (col_hbm, col_ref), (count_hbm, count_ref))
    ):
        index_loads.append(pltpu.make_async_copy(src, dst, index_sems.at[k]))
        index_loads[-1].start()

    barrier = pltpu.get_barrier_semaphore()
    if direct:
        for other in range(1, total):
            pl.semaphore_signal(
                barrier, inc=1, device_id=on_ring((me + other) % total, rows),
                device_id_type=MESH)
        pl.semaphore_wait(barrier, total - 1)
    else:
        for other in (nxt, prv):
            pl.semaphore_signal(barrier, inc=1, device_id=other, device_id_type=MESH)
        pl.semaphore_wait(barrier, 2)

    def remote(src, dst, sems, index, device):
        return pltpu.make_async_remote_copy(
            src_ref=src, dst_ref=dst, send_sem=sems.at[0, index], recv_sem=sems.at[1, index],
            device_id=device, device_id_type=MESH)

    if direct:
        rows_of = width // chips
        here = pl.multiple_of(chip * rows_of, rows_of)

    def scatter(source, landing, sems):
        copies = []
        for o in range(1, chips):
            at = pl.multiple_of(((chip + o) % chips) * rows_of, rows_of)
            copies.append(
                remote(source.at[pl.ds(at, rows_of)], landing.at[o], sems, o, peer(o)))
            copies[-1].start()
        return copies

    def collect(copies, source, landing):
        value = source[pl.ds(here, rows_of)]
        for o in range(1, chips):
            copies[o - 1].wait_recv()
            value = value + landing[o]
        return value

    def gather(target, sems):
        copies = []
        for o in range(1, chips):
            copies.append(remote(
                target.at[pl.ds(here, rows_of)], target.at[pl.ds(here, rows_of)],
                sems, o, peer(o)))
            copies[-1].start()
        return copies

    def gathered(target, sems):
        for o in range(1, chips):
            at = pl.multiple_of(((chip + chips - o) % chips) * rows_of, rows_of)
            remote(target.at[pl.ds(here, rows_of)], target.at[pl.ds(at, rows_of)],
                   sems, o, peer(o)).wait_recv()

    halo = []
    for k in range(chunks):
        loads[k].wait()
        up = remote(window.at[k, pl.ds(edge + inner - edge, edge)],
                    window.at[k, pl.ds(0, edge)], q_sems, 2 * k, nxt)
        down = remote(window.at[k, pl.ds(edge, edge)],
                      window.at[k, pl.ds(edge + inner, edge)], q_sems, 2 * k + 1, prv)
        up.start()
        down.start()
        halo.append((up, down))

    tiles[slots] = jnp.zeros((size, size), BF16)
    tiles_t[slots] = jnp.zeros((size, size), BF16)
    for s in range(slots):
        tile_loads[s].wait()
        tiles_t[s] = tiles[s].T

    for load in index_loads:
        load.wait()
    slot_of = {}
    for row in range(own):
        for off in range(span):
            slot_of[row, off] = jnp.int32(slots)
    for s in range(slots):
        live = s < count_ref[0]
        at_row = row_ref[s] % own
        offset = (col_ref[s] - row_ref[s] + H + tile_total) % tile_total
        for row in range(own):
            for off in range(span):
                hit = live & (at_row == row) & (offset == off)
                slot_of[row, off] = jnp.where(hit, jnp.int32(s), slot_of[row, off])

    def terms(column):
        value = None
        for row in range(own):
            off = column - row
            if 0 <= off < span:
                part = dot(tiles_t[slot_of[row, off]], aq[row], NN)
                value = part if value is None else value + part
        return value

    rim = []
    for k in range(chunks):
        for copy in halo[k]:
            copy.wait_recv()
        for row in range(own):
            value = None
            for off in range(span):
                part = dot(tiles[slot_of[row, off]],
                           window[k, pl.ds((row + off) * size, size)], NN)
                value = part if value is None else value + part
            aq[row] = value.astype(BF16)
        for column in range(H):
            send_lo[k, pl.ds(column * size, size)] = terms(column).astype(BF16)
        down = remote(send_lo.at[k], recv_lo.at[k], y_sems, 2 * k, prv)
        down.start()
        for column in range(H):
            send_hi[k, pl.ds(column * size, size)] = terms(H + own + column).astype(BF16)
        up = remote(send_hi.at[k], recv_hi.at[k], y_sems, 2 * k + 1, nxt)
        up.start()
        rim.append((down, up))
        for column in range(own):
            y[k, pl.ds(column * size, size)] = terms(H + column)

    writes = []
    halves = []
    for k in range(chunks):
        rim[k][1].wait_recv()
        y[k, pl.ds(0, edge)] = y[k, pl.ds(0, edge)] + recv_hi[k].astype(F32)
        rim[k][0].wait_recv()
        y[k, pl.ds(inner - edge, edge)] = (
            y[k, pl.ds(inner - edge, edge)] + recv_lo[k].astype(F32))
        write = pltpu.make_async_copy(y.at[k], y_hbm.at[k], out_sem.at[k])
        write.start()
        writes.append(write)
        high, low = split_high_low(y[k])
        halves.append((high, low))
        for j in range(k + 1):
            jh, jl = halves[j]
            block = dot(jh, high, TN) + (dot(jh, low, TN) + dot(jl, high, TN))
            if not direct:
                acc[k, pl.ds(j * width, width)] = block
                if j != k:
                    acc[j, pl.ds(k * width, width)] = block.T
            elif k == 0:
                acc_first[...] = block
            else:
                acc[j] = block
        if direct and k == 0:
            scatter_first = scatter(acc_first, shards_first, rs_first)

    if direct:
        trade = remote(acc.at[1 - parity], pair, pair_sems, 0, mate)
        trade.start()
        swap[0] = collect(scatter_first, acc_first, shards_first)
        swapped = remote(swap.at[0], swap.at[1], pair_sems, 2, mate)
        swapped.start()
        trade.wait()
        acc[parity] = acc[parity] + pair[...]
        scatter_rest = scatter(acc.at[parity], shards, rs_sems)
        swapped.wait()
        gram_first[pl.ds(here, rows_of)] = swap[0] + swap[1]
        gather_first = gather(gram_first, ag_first)
        gram_ref[parity, pl.ds(here, rows_of)] = collect(scatter_rest, acc.at[parity], shards)
        gather_rest = gather(gram_ref.at[parity], ag_sems)
        gathered(gram_first, ag_first)
        inverse_ref[...] = inverse_factor(gram_first[...] * scale)
        gathered(gram_ref.at[parity], ag_sems)
        back = remote(gram_ref.at[parity], gram_ref.at[parity], pair_sems, 1, mate)
        back.start()
        remote(gram_ref.at[parity], gram_ref.at[1 - parity], pair_sems, 1, mate).wait_recv()
        back.wait_send()
        for copy in scatter_first + gather_first + scatter_rest + gather_rest:
            copy.wait_send()
    else:
        inverse_ref[...] = jnp.zeros_like(inverse_ref)
        gram_ref[...] = acc[...]
    for k in range(chunks):
        for copy in halo[k] + rim[k]:
            copy.wait_send()
        writes[k].wait()


def inverse_factor(a):
    size = a.shape[0]
    groups = size // 8
    parts = [a[8 * i : 8 * i + 8] for i in range(groups)]
    lane = lax.broadcasted_iota(jnp.int32, (8, size), 1)
    sub = lax.broadcasted_iota(jnp.int32, (8, size), 0)

    def row_of(x, at):
        return jnp.broadcast_to(x[at : at + 1], (8, size))

    whole = []
    for home in range(groups):
        first = 8 * home
        later = range(home, groups)
        columns = [
            {i: jnp.broadcast_to(parts[i][:, first + l : first + l + 1], (8, size)) for i in later}
            for l in range(8)
        ]
        mine = parts[home]
        rows = []
        pivots = None
        for j in range(8):
            top = columns[j][home]
            pivot = row_of(top, j)
            inv = 1.0 / pivot
            pivots = pivot if pivots is None else jnp.where(sub == j, pivot, pivots)
            row = jnp.where(lane == first + j, 1.0, row_of(mine, j)) * inv
            rows.append(jnp.where((lane > first + j) & (lane < first + 8), 0.0, row))
            mine = jnp.where(
                sub > j, jnp.where(lane == first + j, 0.0, mine) - top * row, mine)
            for l in range(j + 1, 8):
                weight = row_of(top, l) * inv
                for i in later:
                    columns[l][i] = columns[l][i] - columns[j][i] * weight
        for i in later:
            if i > home:
                value = jnp.where((lane >= first) & (lane < first + 8), 0.0, parts[i])
                for j in range(8):
                    value = value - columns[j][i] * rows[j]
                parts[i] = value
        at = sub + first
        unit = jnp.where(lane < at, mine, jnp.where(lane == at, 1.0, 0.0))
        whole.append(unit * lax.rsqrt(pivots))
    return jnp.concatenate(whole, axis=0)


def solve_kernel(scale, y_hbm, gram_ref, out_hbm, y, out, in_sems, out_sems):
    blocks = y_hbm.shape[0]
    width = y_hbm.shape[2]
    reads = []
    for k in range(blocks):
        reads.append(pltpu.make_async_copy(y_hbm.at[k], y.at[k], in_sems.at[k]))
        reads[-1].start()
    gram = [
        [gram_ref[j, i * width : (i + 1) * width] * scale for j in range(blocks)]
        for i in range(blocks)
    ]
    for read in reads:
        read.wait()
    writes = []
    for k in range(blocks):
        inverse = inverse_factor(gram[k][k])
        basis = dot_split(y[k], inverse, NT)
        out[k] = basis
        write = pltpu.make_async_copy(
            out.at[k], out_hbm.at[:, pl.ds(k * width, width)], out_sems.at[k])
        write.start()
        writes.append(write)
        over = {j: dot(inverse, gram[k][j], NN, EXACT) for j in range(k + 1, blocks)}
        for i in range(k + 1, blocks):
            for j in range(i, blocks):
                gram[i][j] = gram[i][j] - dot(over[i], over[j], TN, EXACT)
            y[i] = y[i] - dot_split(basis, over[i], NN)
    for write in writes:
        write.wait()


def finish_kernel(scale, y_hbm, gram_ref, inverse_ref, out_hbm, y, out, in_sems, out_sems):
    width = y_hbm.shape[2]

    def read(k):
        return pltpu.make_async_copy(y_hbm.at[k], y.at[k], in_sems.at[k])

    def write(k):
        return pltpu.make_async_copy(
            out.at[k], out_hbm.at[:, pl.ds(k * width, width)], out_sems.at[k])

    for k in range(2):
        read(k).start()
    first = inverse_ref[...]
    over = dot(first, gram_ref[0] * scale, NN, EXACT)
    rest = gram_ref[1] * scale - dot(over, over, TN, EXACT)
    read(0).wait()
    basis = dot_split(y[0], first, NT)
    out[0] = basis
    write(0).start()
    read(1).wait()
    y[1] = y[1] - dot_split(basis, over, NN)
    out[1] = dot_split(y[1], inverse_factor(rest), NT)
    write(1).start()
    for k in range(2):
        write(k).wait()


def on_device(tiles, tile_row, tile_col, tile_count, q_block):
    slots, size, unused_size = tiles.shape
    height, basis = q_block.shape
    groups, rows = lax.axis_size("grp"), lax.axis_size("row")
    total = groups * rows
    own = height // size
    tile_total = own * total
    width = BLOCK
    chunks = basis // width
    edge = H * size
    chips = max(total // 2, 1)
    direct = (
        total <= DIRECT_LIMIT and rows % 2 == 0 and chunks == 2 and width % (8 * chips) == 0
    )
    shard = width // chips if direct else 8
    partners = chips if direct else 1
    reduced = (chunks, width if direct else basis, width)
    scale = 1.0 / (height * total)
    any_spec = pl.BlockSpec(memory_space=pl.ANY)
    vmem_spec = pl.BlockSpec(memory_space=pltpu.VMEM)
    hbm_spec = pl.BlockSpec(memory_space=pltpu.HBM)
    dma = pltpu.SemaphoreType.DMA
    y, gram, inverse = pl.pallas_call(
        functools.partial(step_kernel, direct, scale, groups, rows, tile_total),
        out_shape=(
            jax.ShapeDtypeStruct((chunks, height, width), F32),
            jax.ShapeDtypeStruct(reduced, F32),
            jax.ShapeDtypeStruct((width, width), F32),
        ),
        in_specs=[hbm_spec] * 5,
        out_specs=(any_spec, vmem_spec, vmem_spec),
        scratch_shapes=[
            pltpu.SMEM(tile_row.shape, jnp.int32),
            pltpu.SMEM(tile_col.shape, jnp.int32),
            pltpu.SMEM(tile_count.shape, jnp.int32),
            pltpu.VMEM((chunks, height + 2 * edge, width), BF16),
            pltpu.VMEM((slots + 1, size, size), BF16),
            pltpu.VMEM((slots + 1, size, size), BF16),
            pltpu.VMEM((own, size, width), BF16),
            pltpu.VMEM((chunks, edge, width), BF16),
            pltpu.VMEM((chunks, edge, width), BF16),
            pltpu.VMEM((chunks, edge, width), BF16),
            pltpu.VMEM((chunks, edge, width), BF16),
            pltpu.VMEM((chunks, height, width), F32),
            pltpu.VMEM(reduced, F32),
            pltpu.VMEM(reduced[1:], F32),
            pltpu.VMEM((partners, shard, width), F32),
            pltpu.VMEM((width, width), F32),
            pltpu.VMEM((width, width), F32),
            pltpu.VMEM((partners, shard, width), F32),
            pltpu.VMEM((2, shard, width), F32),
            dma((slots + chunks,)),
            dma((2, 2 * chunks)),
            dma((2, 2 * chunks)),
            dma((2, 3)),
            dma((2, partners)),
            dma((2, partners)),
            dma((2, partners)),
            dma((2, partners)),
            dma((chunks,)),
            dma((3,)),
        ],
        compiler_params=pltpu.CompilerParams(
            collective_id=0, has_side_effects=True, vmem_limit_bytes=VMEM_LIMIT
        ),
    )(tile_row, tile_col, tile_count, tiles, q_block)
    if not direct:
        gram = lax.psum(gram, ("grp", "row"))
    last = finish_kernel if direct else solve_kernel
    operands = (y, gram, inverse) if direct else (y, gram)
    return pl.pallas_call(
        functools.partial(last, scale),
        out_shape=jax.ShapeDtypeStruct((height, basis), F32),
        in_specs=[any_spec] + [vmem_spec] * (len(operands) - 1),
        out_specs=any_spec,
        scratch_shapes=[
            pltpu.VMEM((chunks, height, width), F32),
            pltpu.VMEM((chunks, height, width), F32),
            dma((chunks,)),
            dma((chunks,)),
        ],
        compiler_params=pltpu.CompilerParams(vmem_limit_bytes=VMEM_LIMIT),
    )(*operands)


def solution(mesh):
    placed = (
        P(("grp", "row"), None, None),
        P(("grp", "row")),
        P(("grp", "row")),
        P(("grp", "row")),
        P(("grp", "row"), None),
    )
    return jax.shard_map(
        on_device, mesh=mesh, in_specs=placed, out_specs=P(("grp", "row"), None), check_vma=False
    )
```

```python
import functools

import jax
import jax.numpy as jnp
from jax import lax
from jax.experimental import pallas as pl
from jax.experimental.pallas import tpu as pltpu
from jax.sharding import PartitionSpec as P

H = 2
BLOCK = 128
CHUNKS = 2
DIRECT_LIMIT = 32
VMEM_LIMIT = 67_043_328
MESH = pl.DeviceIdType.MESH
F32 = jnp.float32
BF16 = jnp.bfloat16
EXACT = lax.Precision.HIGHEST


def split_high_low(x):
    high = x.astype(BF16)
    return high, (x - high.astype(F32)).astype(BF16)


def dot(a, b, dims, precision=None):
    return lax.dot_general(
        a, b, (dims, ((), ())), precision=precision, preferred_element_type=F32
    )


NN = ((1,), (0,))
NT = ((1,), (1,))
TN = ((0,), (0,))


def dot_split(x, m, dims):
    xh, xl = split_high_low(x)
    mh, ml = split_high_low(m)
    return dot(xh, mh, dims) + (dot(xl, mh, dims) + dot(xh, ml, dims))


def on_ring(device, rows):
    return (device // rows, device % rows)


def step_kernel(
    direct, scale, groups, rows, tile_total,
    row_hbm, col_hbm, count_hbm, tiles_hbm, q_hbm,
    y_hbm, gram_ref, inverse_ref,
    row_ref, col_ref, count_ref, window, tiles, tiles_t, aq, send_lo, send_hi, recv_lo, recv_hi, y, acc, pair, shards,
    acc_first, gram_first, shards_first, swap, kept, load_sems, q_sems, y_sems, pair_sems, rs_sems, ag_sems, rs_first, ag_first, out_sem, index_sems,
):
    slots = tiles_hbm.shape[0]
    size = tiles_hbm.shape[1]
    own = q_hbm.shape[0] // size
    chunks = window.shape[0]
    width = window.shape[2]
    span = 2 * H + 1
    edge = H * size
    inner = own * size
    total = groups * rows
    g, r = lax.axis_index("grp"), lax.axis_index("row")
    me = g * rows + r
    nxt = on_ring((me + 1) % total, rows)
    prv = on_ring((me + total - 1) % total, rows)
    chips = total // 2
    parity = r % 2
    chip = me // 2
    mate = on_ring(chip * 2 + (1 - parity), rows)

    def peer(offset):
        return on_ring(((chip + offset) % chips) * 2 + parity, rows)

    loads = []
    for k in range(chunks):
        loads.append(pltpu.make_async_copy(
            q_hbm.at[:, pl.ds(k * width, width)],
            window.at[k, pl.ds(edge, inner)], load_sems.at[slots + k]))
        loads[-1].start()
    tile_loads = []
    for s in range(slots):
        tile_loads.append(pltpu.make_async_copy(tiles_hbm.at[s], tiles.at[s], load_sems.at[s]))
        tile_loads[-1].start()

    index_loads = []
    for k, (src, dst) in enumerate(
        ((row_hbm, row_ref), (col_hbm, col_ref), (count_hbm, count_ref))
    ):
        index_loads.append(pltpu.make_async_copy(src, dst, index_sems.at[k]))
        index_loads[-1].start()

    barrier = pltpu.get_barrier_semaphore()
    if direct:
        for other in range(1, total):
            pl.semaphore_signal(
                barrier, inc=1, device_id=on_ring((me + other) % total, rows),
                device_id_type=MESH)
        pl.semaphore_wait(barrier, total - 1)
    else:
        for other in (nxt, prv):
            pl.semaphore_signal(barrier, inc=1, device_id=other, device_id_type=MESH)
        pl.semaphore_wait(barrier, 2)

    def remote(src, dst, sems, index, device):
        return pltpu.make_async_remote_copy(
            src_ref=src, dst_ref=dst, send_sem=sems.at[0, index], recv_sem=sems.at[1, index],
            device_id=device, device_id_type=MESH)

    if direct:
        rows_of = width // chips
        here = pl.multiple_of(chip * rows_of, rows_of)

    def scatter(source, landing, sems):
        copies = []
        for o in range(1, chips):
            at = pl.multiple_of(((chip + o) % chips) * rows_of, rows_of)
            copies.append(
                remote(source.at[pl.ds(at, rows_of)], landing.at[o], sems, o, peer(o)))
            copies[-1].start()
        return copies

    def collect(copies, source, landing):
        value = source[pl.ds(here, rows_of)]
        for o in range(1, chips):
            copies[o - 1].wait_recv()
            value = value + landing[o]
        return value

    def gather(target, sems):
        copies = []
        for o in range(1, chips):
            copies.append(remote(
                target.at[pl.ds(here, rows_of)], target.at[pl.ds(here, rows_of)],
                sems, o, peer(o)))
            copies[-1].start()
        return copies

    def gathered(target, sems):
        for o in range(1, chips):
            at = pl.multiple_of(((chip + chips - o) % chips) * rows_of, rows_of)
            remote(target.at[pl.ds(here, rows_of)], target.at[pl.ds(at, rows_of)],
                   sems, o, peer(o)).wait_recv()

    halo = []
    for k in range(chunks):
        loads[k].wait()
        up = remote(window.at[k, pl.ds(edge + inner - edge, edge)],
                    window.at[k, pl.ds(0, edge)], q_sems, 2 * k, nxt)
        down = remote(window.at[k, pl.ds(edge, edge)],
                      window.at[k, pl.ds(edge + inner, edge)], q_sems, 2 * k + 1, prv)
        up.start()
        down.start()
        halo.append((up, down))

    tiles[slots] = jnp.zeros((size, size), BF16)
    tiles_t[slots] = jnp.zeros((size, size), BF16)
    for s in range(slots):
        tile_loads[s].wait()
        tiles_t[s] = tiles[s].T

    for load in index_loads:
        load.wait()
    slot_of = {}
    for row in range(own):
        for off in range(span):
            slot_of[row, off] = jnp.int32(slots)
    for s in range(slots):
        live = s < count_ref[0]
        at_row = row_ref[s] % own
        offset = (col_ref[s] - row_ref[s] + H + tile_total) % tile_total
        for row in range(own):
            for off in range(span):
                hit = live & (at_row == row) & (offset == off)
                slot_of[row, off] = jnp.where(hit, jnp.int32(s), slot_of[row, off])

    def terms(column):
        value = None
        for row in range(own):
            off = column - row
            if 0 <= off < span:
                part = dot(tiles_t[slot_of[row, off]], aq[row], NN)
                value = part if value is None else value + part
        return value

    rim = []
    for k in range(chunks):
        for copy in halo[k]:
            copy.wait_recv()
        for row in range(own):
            value = None
            for off in range(span):
                part = dot(tiles[slot_of[row, off]],
                           window[k, pl.ds((row + off) * size, size)], NN)
                value = part if value is None else value + part
            aq[row] = value.astype(BF16)
        for column in range(H):
            send_lo[k, pl.ds(column * size, size)] = terms(column).astype(BF16)
        down = remote(send_lo.at[k], recv_lo.at[k], y_sems, 2 * k, prv)
        down.start()
        for column in range(H):
            send_hi[k, pl.ds(column * size, size)] = terms(H + own + column).astype(BF16)
        up = remote(send_hi.at[k], recv_hi.at[k], y_sems, 2 * k + 1, nxt)
        up.start()
        rim.append((down, up))
        for column in range(own):
            y[k, pl.ds(column * size, size)] = terms(H + column)

    writes = []
    halves = []
    for k in range(chunks):
        rim[k][1].wait_recv()
        y[k, pl.ds(0, edge)] = y[k, pl.ds(0, edge)] + recv_hi[k].astype(F32)
        rim[k][0].wait_recv()
        y[k, pl.ds(inner - edge, edge)] = (
            y[k, pl.ds(inner - edge, edge)] + recv_lo[k].astype(F32))
        write = pltpu.make_async_copy(y.at[k], y_hbm.at[k], out_sem.at[k])
        write.start()
        writes.append(write)
        high, low = split_high_low(y[k])
        high_t = high.T
        cross = dot(high_t, low, NN)
        for j in range(k + 1):
            if j == k:
                block = dot(high_t, high, NN) + (cross + cross.T)
            else:
                block = dot(halves[j][0][...], high, NN) + (
                    dot(halves[j][0][...], low, NN) + dot(halves[j][1][...], high, NN))
            if not direct:
                acc[k, pl.ds(j * width, width)] = block
                if j != k:
                    acc[j, pl.ds(k * width, width)] = block.T
            elif k == 0:
                acc_first[...] = block
            else:
                acc[j] = block
        if direct and k == 0:
            scatter_first = scatter(acc_first, shards_first, rs_first)
        if k + 1 < chunks:
            kept[2 * k] = high_t
            kept[2 * k + 1] = low.T
            halves.append((kept.at[2 * k], kept.at[2 * k + 1]))

    if direct:
        trade = remote(acc.at[1 - parity], pair, pair_sems, 0, mate)
        trade.start()
        swap[0] = collect(scatter_first, acc_first, shards_first)
        swapped = remote(swap.at[0], swap.at[1], pair_sems, 2, mate)
        swapped.start()
        trade.wait()
        acc[parity] = acc[parity] + pair[...]
        scatter_rest = scatter(acc.at[parity], shards, rs_sems)
        swapped.wait()
        gram_first[pl.ds(here, rows_of)] = swap[0] + swap[1]
        gather_first = gather(gram_first, ag_first)
        gram_ref[parity, pl.ds(here, rows_of)] = collect(scatter_rest, acc.at[parity], shards)
        gather_rest = gather(gram_ref.at[parity], ag_sems)
        gathered(gram_first, ag_first)
        inverse_ref[...] = inverse_factor(gram_first[...] * scale)
        gathered(gram_ref.at[parity], ag_sems)
        back = remote(gram_ref.at[parity], gram_ref.at[parity], pair_sems, 1, mate)
        back.start()
        remote(gram_ref.at[parity], gram_ref.at[1 - parity], pair_sems, 1, mate).wait_recv()
        back.wait_send()
        for copy in scatter_first + gather_first + scatter_rest + gather_rest:
            copy.wait_send()
    else:
        inverse_ref[...] = jnp.zeros_like(inverse_ref)
        gram_ref[...] = acc[...]
    for k in range(chunks):
        for copy in halo[k] + rim[k]:
            copy.wait_send()
        writes[k].wait()


def inverse_factor(a):
    size = a.shape[0]
    groups = size // 8
    parts = [a[8 * i : 8 * i + 8] for i in range(groups)]
    lane = lax.broadcasted_iota(jnp.int32, (8, size), 1)
    sub = lax.broadcasted_iota(jnp.int32, (8, size), 0)

    def row_of(x, at):
        return jnp.broadcast_to(x[at : at + 1], (8, size))

    whole = []
    for home in range(groups):
        first = 8 * home
        later = range(home, groups)
        columns = [
            {i: jnp.broadcast_to(parts[i][:, first + l : first + l + 1], (8, size)) for i in later}
            for l in range(8)
        ]
        mine = parts[home]
        rows = []
        pivots = None
        for j in range(8):
            top = columns[j][home]
            pivot = row_of(top, j)
            inv = 1.0 / pivot
            pivots = pivot if pivots is None else jnp.where(sub == j, pivot, pivots)
            row = jnp.where(lane == first + j, 1.0, row_of(mine, j)) * inv
            rows.append(jnp.where((lane > first + j) & (lane < first + 8), 0.0, row))
            mine = jnp.where(
                sub > j, jnp.where(lane == first + j, 0.0, mine) - top * row, mine)
            for l in range(j + 1, 8):
                weight = row_of(top, l) * inv
                for i in later:
                    columns[l][i] = columns[l][i] - columns[j][i] * weight
        for i in later:
            if i > home:
                value = jnp.where((lane >= first) & (lane < first + 8), 0.0, parts[i])
                for j in range(8):
                    value = value - columns[j][i] * rows[j]
                parts[i] = value
        at = sub + first
        unit = jnp.where(lane < at, mine, jnp.where(lane == at, 1.0, 0.0))
        whole.append(unit * lax.rsqrt(pivots))
    return jnp.concatenate(whole, axis=0)


def solve_kernel(scale, y_hbm, gram_ref, out_hbm, y, out, in_sems, out_sems):
    blocks = y_hbm.shape[0]
    width = y_hbm.shape[2]
    reads = []
    for k in range(blocks):
        reads.append(pltpu.make_async_copy(y_hbm.at[k], y.at[k], in_sems.at[k]))
        reads[-1].start()
    gram = [
        [gram_ref[j, i * width : (i + 1) * width] * scale for j in range(blocks)]
        for i in range(blocks)
    ]
    for read in reads:
        read.wait()
    writes = []
    for k in range(blocks):
        inverse = inverse_factor(gram[k][k])
        basis = dot_split(y[k], inverse, NT)
        out[k] = basis
        write = pltpu.make_async_copy(
            out.at[k], out_hbm.at[:, pl.ds(k * width, width)], out_sems.at[k])
        write.start()
        writes.append(write)
        over = {j: dot(inverse, gram[k][j], NN, EXACT) for j in range(k + 1, blocks)}
        for i in range(k + 1, blocks):
            for j in range(i, blocks):
                gram[i][j] = gram[i][j] - dot(over[i], over[j], TN, EXACT)
            y[i] = y[i] - dot_split(basis, over[i], NN)
    for write in writes:
        write.wait()


def finish_kernel(scale, y_hbm, gram_ref, inverse_ref, out_hbm, y, out, in_sems, out_sems):
    width = y_hbm.shape[2]

    def read(k):
        return pltpu.make_async_copy(y_hbm.at[k], y.at[k], in_sems.at[k])

    def write(k):
        return pltpu.make_async_copy(
            out.at[k], out_hbm.at[:, pl.ds(k * width, width)], out_sems.at[k])

    for k in range(2):
        read(k).start()
    first = inverse_ref[...]
    over = dot(first, gram_ref[0] * scale, NN, EXACT)
    rest = gram_ref[1] * scale - dot(over, over, TN, EXACT)
    read(0).wait()
    basis = dot_split(y[0], first, NT)
    out[0] = basis
    write(0).start()
    read(1).wait()
    y[1] = y[1] - dot_split(basis, over, NN)
    out[1] = dot_split(y[1], inverse_factor(rest), NT)
    write(1).start()
    for k in range(2):
        write(k).wait()


def on_device(tiles, tile_row, tile_col, tile_count, q_block):
    slots, size, unused_size = tiles.shape
    height, basis = q_block.shape
    groups, rows = lax.axis_size("grp"), lax.axis_size("row")
    total = groups * rows
    own = height // size
    tile_total = own * total
    width = BLOCK
    chunks = basis // width
    edge = H * size
    chips = max(total // 2, 1)
    direct = (
        total <= DIRECT_LIMIT and rows % 2 == 0 and chunks == 2 and width % (8 * chips) == 0
    )
    shard = width // chips if direct else 8
    partners = chips if direct else 1
    reduced = (chunks, width if direct else basis, width)
    scale = 1.0 / (height * total)
    any_spec = pl.BlockSpec(memory_space=pl.ANY)
    vmem_spec = pl.BlockSpec(memory_space=pltpu.VMEM)
    hbm_spec = pl.BlockSpec(memory_space=pltpu.HBM)
    dma = pltpu.SemaphoreType.DMA
    y, gram, inverse = pl.pallas_call(
        functools.partial(step_kernel, direct, scale, groups, rows, tile_total),
        out_shape=(
            jax.ShapeDtypeStruct((chunks, height, width), F32),
            jax.ShapeDtypeStruct(reduced, F32),
            jax.ShapeDtypeStruct((width, width), F32),
        ),
        in_specs=[hbm_spec] * 5,
        out_specs=(any_spec, vmem_spec, vmem_spec),
        scratch_shapes=[
            pltpu.SMEM(tile_row.shape, jnp.int32),
            pltpu.SMEM(tile_col.shape, jnp.int32),
            pltpu.SMEM(tile_count.shape, jnp.int32),
            pltpu.VMEM((chunks, height + 2 * edge, width), BF16),
            pltpu.VMEM((slots + 1, size, size), BF16),
            pltpu.VMEM((slots + 1, size, size), BF16),
            pltpu.VMEM((own, size, width), BF16),
            pltpu.VMEM((chunks, edge, width), BF16),
            pltpu.VMEM((chunks, edge, width), BF16),
            pltpu.VMEM((chunks, edge, width), BF16),
            pltpu.VMEM((chunks, edge, width), BF16),
            pltpu.VMEM((chunks, height, width), F32),
            pltpu.VMEM(reduced, F32),
            pltpu.VMEM(reduced[1:], F32),
            pltpu.VMEM((partners, shard, width), F32),
            pltpu.VMEM((width, width), F32),
            pltpu.VMEM((width, width), F32),
            pltpu.VMEM((partners, shard, width), F32),
            pltpu.VMEM((2, shard, width), F32),
            pltpu.VMEM((2 * chunks, width, height), BF16),
            dma((slots + chunks,)),
            dma((2, 2 * chunks)),
            dma((2, 2 * chunks)),
            dma((2, 3)),
            dma((2, partners)),
            dma((2, partners)),
            dma((2, partners)),
            dma((2, partners)),
            dma((chunks,)),
            dma((3,)),
        ],
        compiler_params=pltpu.CompilerParams(
            collective_id=0, has_side_effects=True, vmem_limit_bytes=VMEM_LIMIT
        ),
    )(tile_row, tile_col, tile_count, tiles, q_block)
    if not direct:
        gram = lax.psum(gram, ("grp", "row"))
    last = finish_kernel if direct else solve_kernel
    operands = (y, gram, inverse) if direct else (y, gram)
    return pl.pallas_call(
        functools.partial(last, scale),
        out_shape=jax.ShapeDtypeStruct((height, basis), F32),
        in_specs=[any_spec] + [vmem_spec] * (len(operands) - 1),
        out_specs=any_spec,
        scratch_shapes=[
            pltpu.VMEM((chunks, height, width), F32),
            pltpu.VMEM((chunks, height, width), F32),
            dma((chunks,)),
            dma((chunks,)),
        ],
        compiler_params=pltpu.CompilerParams(vmem_limit_bytes=VMEM_LIMIT),
    )(*operands)


def solution(mesh):
    placed = (
        P(("grp", "row"), None, None),
        P(("grp", "row")),
        P(("grp", "row")),
        P(("grp", "row")),
        P(("grp", "row"), None),
    )
    return jax.shard_map(
        on_device, mesh=mesh, in_specs=placed, out_specs=P(("grp", "row"), None), check_vma=False
    )
```
